32 devices in a mesh: rep: 2 (over x), pts: 16 (over z, y, core).
Axes of the slice: x: 2, y: 2, z: 4, core: 2. Of those that a mesh axis runs over, the one named last changes fastest.
Arguments:
- orbitals: bfloat16 [64, 32, 512], P(('rep', 'pts')), parts along dimension 0, may hold values from -6 to 6
- points: bfloat16 [12288, 512], P('pts'), may hold values from -0.25 to 0.25
- coupling: bfloat16 [12288, 4096], P('pts'), may hold values from -0.01953125 to 0.01953125
- fields: int32 [64, 4096], P('rep'), parts along dimension 0, may hold values from 0 to 3
- destination: int32 [64], P('rep'), parts along dimension 0, may hold values from 0 to 15, as said below
Outputs:
- moved: bfloat16 [96, 32, 512], P(('rep', 'pts')), parts along dimension 0
The draws below stay inside these ranges and needn't reach their ends.
There are 2 independent parts, one for each index of `rep`. The reference program is written for one: setup_inputs(seed, part) draws one part's arguments, and reference() takes and returns one part's arrays. A program takes and returns all parts, laid end to end along the dimension named above; an argument that names none is the same for every part. Nothing has to cross between parts.
Inputs may be any that keep to these rules, and one draw needn't show every extreme that they name: Each group is the destination of at most 3 walkers; some group receives exactly 3, and the 2 walkers of some group all go to it.
All inputs are finite; a program needn't handle non-finite values.
Results may differ from the reference program's by a relative error of at most 0.008.
Values may be sent and summed in bfloat16 or wider, within the bound.
No kernel may reach another device: no remote copies, remote signals or barrier semaphores. Data moves between devices by JAX's collectives and lax.ppermute only.
A program may use at most 64 MiB of HBM per device.

```python
import jax
import jax.numpy as jnp
from jax import lax

N_ORB = 512
NOCC = 16
NPTS = 12288
NFIELD = 4096
W_DEV = 2
CAP = 3
WALKERS = 32
N_PTS = 16


def draw_destination(key, part):
    slots_all = N_PTS * CAP
    count_all = W_DEV * N_PTS
    group_key = jax.random.fold_in(key, 11)
    noise_key = jax.random.fold_in(key, 12)
    offset_key = jax.random.fold_in(key, 13)
    chosen_group = jax.random.randint(group_key, (), 0, N_PTS)
    noise = jax.random.randint(noise_key, (slots_all,), 0, 1 << 16)
    slot_ids = jnp.arange(slots_all, dtype=jnp.int32)
    scores = noise * slots_all + slot_ids
    scores = jnp.where(slot_ids // CAP == chosen_group, slot_ids - slots_all, scores)
    ordering = jnp.argsort(scores, stable=True).astype(jnp.int32)
    picked = ordering[:count_all] // CAP
    offset = jax.random.randint(offset_key, (), 0, N_PTS) * W_DEV
    return jnp.roll(picked, offset).astype(jnp.int32)


def place_ends(drawn, own_key, least, largest):
    longest = drawn.shape.index(max(drawn.shape))
    spots = []
    for shift in (0, 1):
        where = [jax.random.randint(jax.random.fold_in(own_key, axis), (), 0, length) for axis, length in enumerate(drawn.shape)]
        where[longest] = (where[longest] + shift) % drawn.shape[longest]
        spots.append(tuple(where))
    return drawn.at[spots[0]].set(least).at[spots[1]].set(largest)


def steps_of(own_key, extent, split, least, high):
    gain, own = 1.0, jax.random.fold_in(own_key, 6)
    for position, parts in split:
        heights = jnp.exp(jax.random.uniform(jax.random.fold_in(own, position), (parts,), jnp.float32, least / len(split), high / len(split)))
        gain = gain * jnp.repeat(heights, extent[position] // parts).reshape([-1 if axis == position else 1 for axis in range(len(extent))])
    return gain


def centred(stream_key, extent, spread, most, shards=(), kind=jnp.bfloat16):
    array = jax.random.normal(stream_key, extent, jnp.float32) * spread
    if len(shards) > 0:
        array = steps_of(stream_key, extent, shards, -0.22, 0.18) * array
    return jnp.clip(array, min=-most, max=most).astype(kind)


def setup_inputs(seed: int = 0, part: int = 0) -> dict:
    streams_of = jax.random.split(jax.random.key(seed), 6)
    part_keys = jax.random.split(jax.random.fold_in(streams_of[5], part), 6)
    orbitals = centred(part_keys[0], (WALKERS, 2 * NOCC, N_ORB), 1.0, 6.0, ((0, 16),))
    points = centred(streams_of[1], (NPTS, N_ORB), N_ORB ** -0.5, 0.25, ((0, 16),))
    coupling = centred(streams_of[2], (NPTS, NFIELD), (0.09 * NFIELD ** -0.5), 0.01953125, ((0, 16),))
    fields = place_ends(jax.random.randint(part_keys[3], (WALKERS, NFIELD), 0, 4), jax.random.fold_in(part_keys[3], 1), 0, 3).astype(jnp.int32)
    destination = draw_destination(jax.random.fold_in(jax.random.fold_in(streams_of[5], part), 71), part)
    return {"orbitals": orbitals, "points": points, "coupling": coupling, "fields": fields, "destination": destination}


LEVELS = (-2.3344142183389773, -0.7419637843027258, 0.7419637843027258, 2.3344142183389773)


def field_values(fields):
    values = jnp.zeros(fields.shape, jnp.float32)
    for level_index in range(4):
        values = values + jnp.where(fields == level_index, LEVELS[level_index], 0.0)
    return values.astype(jnp.bfloat16)


def rotate(block):
    half_rows = block.shape[-2] // 2
    return jnp.concatenate([-block[..., half_rows:, :], block[..., :half_rows, :]], axis=-2)


def apply_field(rows, points, scale):
    table = points.astype(jnp.float32)
    inner = jnp.einsum('wrn,pn->wrp', rows.astype(jnp.float32), table)
    scaled = lax.optimization_barrier((inner * scale[:, None, :]).astype(jnp.bfloat16))
    return rotate(jnp.einsum('wrp,pn->wrn', scaled.astype(jnp.float32), table))


def reference(orbitals, points, coupling, fields, destination):
    values = field_values(fields)
    scale = jnp.dot(values, coupling.T, preferred_element_type=jnp.float32)
    first = apply_field(orbitals, points, scale)
    first_rounded = lax.optimization_barrier(first.astype(jnp.bfloat16))
    second = 0.5 * apply_field(first_rounded, points, scale)
    propagated = (orbitals.astype(jnp.float32) + first + second).astype(jnp.bfloat16)
    walker_ids = jnp.arange(destination.shape[0], dtype=jnp.int32)
    earlier = (destination[:, None] == destination[None, :]) & (walker_ids[None, :] < walker_ids[:, None])
    target = destination * CAP + jnp.sum(earlier.astype(jnp.int32), axis=1).astype(jnp.int32)
    moved = jnp.zeros((N_PTS * CAP,) + propagated.shape[1:], jnp.bfloat16)
    return moved.at[target].set(propagated)
```

```python
import functools

import jax
import jax.numpy as jnp
from jax import lax
from jax.experimental import pallas as pl
from jax.experimental.pallas import tpu as pltpu
from jax.sharding import PartitionSpec as P

LEVELS = (-2.3344142183389773, -0.7419637843027258, 0.7419637843027258, 2.3344142183389773)
VMEM = pl.BlockSpec(memory_space=pltpu.VMEM)
SMEM = pl.BlockSpec(memory_space=pltpu.SMEM)
PARAMS = pltpu.CompilerParams(vmem_limit_bytes=40 * 1024 * 1024)


def field_values(fields):
    values = jnp.zeros(fields.shape, jnp.float32)
    for level_index in range(4):
        values = values + jnp.where(fields == level_index, LEVELS[level_index], 0.0)
    return values.astype(jnp.bfloat16)


def swap(block, offset):
    count = lax.axis_size("pts")
    return lax.ppermute(block, "pts", [(i, i ^ offset) for i in range(count)])


def fill_sources(dest_ref, source_ref, seen_ref, slot_count):
    def clear_slot(i, _):
        source_ref[i] = -1
        return 0

    def clear_seen(i, _):
        seen_ref[i] = 0
        return 0

    def place(walker, _):
        group = dest_ref[walker]
        rank = seen_ref[group]
        seen_ref[group] = rank + 1
        source_ref[group * slot_count + rank] = walker
        return 0

    lax.fori_loop(0, source_ref.shape[0], clear_slot, 0)
    lax.fori_loop(0, seen_ref.shape[0], clear_seen, 0)
    lax.fori_loop(0, dest_ref.shape[0], place, 0)


def scale_slots_kernel(slot_count, group_count, dest_ref, me_ref, scale_ref, out_ref, source_ref, seen_ref):
    fill_sources(dest_ref, source_ref, seen_ref, slot_count)
    half = group_count // 2
    top = me_ref[0] // half
    for group in range(half):
        for member in range(2):
            owner = (top ^ member) * half + group
            for k in range(slot_count):
                walker = jnp.maximum(source_ref[owner * slot_count + k], 0)
                row = scale_ref[pl.ds(walker, 1), :]
                out_ref[group, pl.ds(member * slot_count + k, 1), :] = row


def slot_scales(scale, destination, me, slot_count, group_count):
    slots = 2 * slot_count
    return pl.pallas_call(
        functools.partial(scale_slots_kernel, slot_count, group_count),
        out_shape=jax.ShapeDtypeStruct((group_count // 2, slots, scale.shape[1]), jnp.float32),
        in_specs=[SMEM, SMEM, VMEM],
        out_specs=VMEM,
        scratch_shapes=[
            pltpu.SMEM((group_count * slot_count,), jnp.int32),
            pltpu.SMEM((group_count,), jnp.int32),
        ],
        compiler_params=PARAMS,
        name="slot_scales",
    )(destination, me, scale)


def place_kernel(slot_count, group_count, own_count, order, dest_ref, me_ref, near_ref, far_ref, out_ref, source_ref, seen_ref):
    fill_sources(dest_ref, source_ref, seen_ref, slot_count)
    half = group_count // 2
    me = me_ref[0]
    for member in range(2):
        for k in range(slot_count):
            owner = me ^ (half * member)
            walker = source_ref[owner * slot_count + k]
            slot = member * slot_count + k

            @pl.when(walker < 0)
            def _():
                out_ref[slot] = jnp.zeros(out_ref.shape[1:], out_ref.dtype)

            @pl.when(walker >= 0)
            def _():
                offset = (walker // own_count) ^ me
                place = jnp.int32(0)
                for step, bit in enumerate(order):
                    place = place + ((offset // bit) & 1) * (1 << step)
                place = place * own_count + walker % own_count

                @pl.when((offset & 1) == 0)
                def _():
                    out_ref[slot] = near_ref[place]

                @pl.when((offset & 1) == 1)
                def _():
                    out_ref[slot] = far_ref[place]


def place_orbitals(near, far, destination, me, slot_count, group_count, own_count, order):
    slots = 2 * slot_count
    return pl.pallas_call(
        functools.partial(place_kernel, slot_count, group_count, own_count, order),
        out_shape=jax.ShapeDtypeStruct((slots,) + near.shape[1:], near.dtype),
        in_specs=[SMEM, SMEM, VMEM, VMEM],
        out_specs=VMEM,
        scratch_shapes=[
            pltpu.SMEM((group_count * slot_count,), jnp.int32),
            pltpu.SMEM((group_count,), jnp.int32),
        ],
        compiler_params=PARAMS,
        name="place_orbitals",
    )(destination, me, near, far)


def image_of(rows, low, scale_ref, pieces):
    slots, per_slot, orbs = rows.shape
    flat = rows.reshape(slots * per_slot, orbs)
    total = jnp.zeros((slots * per_slot, orbs), jnp.float32)
    for offset, begin, ref in pieces:
        table = ref[...]
        count = table.shape[0]
        inner = lax.dot_general(flat, table, (((1,), (1,)), ((), ())), preferred_element_type=jnp.float32)
        scale = scale_ref[low ^ offset][:, begin:begin + count]
        scaled = inner.reshape(slots, per_slot, count) * scale[:, None, :]
        scaled = scaled.astype(jnp.bfloat16).reshape(slots * per_slot, count)
        total = total + jnp.dot(scaled, table, preferred_element_type=jnp.float32)
    return total.reshape(slots, per_slot, orbs)


def image_kernel(keys, low_ref, rows_ref, scale_ref, *refs):
    out_ref = refs[-1]
    low = low_ref[0]
    pieces = [(offset, begin, ref) for (offset, begin), ref in zip(keys, refs)]
    out_ref[...] = image_of(rows_ref[...], low, scale_ref, pieces)


def image(rows, low, scales, pieces, name):
    keys = [key for key, _ in pieces]
    points_count = sum(p.shape[0] for _, p in pieces)
    flops = 4 * rows.shape[0] * rows.shape[1] * rows.shape[2] * points_count
    return pl.pallas_call(
        functools.partial(image_kernel, keys),
        out_shape=jax.ShapeDtypeStruct(rows.shape, jnp.float32),
        in_specs=[SMEM] + [VMEM] * (2 + len(pieces)),
        out_specs=VMEM,
        compiler_params=PARAMS,
        cost_estimate=pl.CostEstimate(flops=flops, bytes_accessed=points_count * rows.shape[2] * 2, transcendentals=0),
        name=name,
    )(low, rows, scales, *[p for _, p in pieces])


def rotate(block):
    half_rows = block.shape[-2] // 2
    return jnp.concatenate([-block[..., half_rows:, :], block[..., :half_rows, :]], axis=-2)


def gather_points(points, half):
    early, late = [((0, 0), points)], []
    bits = []
    bit = 2
    while bit < half:
        bits.append(bit)
        bit *= 2
    if len(bits) >= 2:
        one, two = bits[:2]
        middle = points.shape[0] // 2
        over_one = swap(points, one)
        over_two = swap(points, two)
        early += [((one, 0), over_one), ((two, 0), over_two)]
        late += [((one ^ two, 0), swap(over_one[:middle], two)), ((one ^ two, middle), swap(over_two[middle:], one))]
        bits = bits[2:]
    for bit in bits:
        late += [((m ^ bit, begin), swap(rows, bit)) for (m, begin), rows in early + late]
    far = lambda pieces: [((m ^ 1, begin), swap(rows, 1)) for (m, begin), rows in pieces]
    return early + far(early), late + far(late)


def per_device(orbitals, points, coupling, fields, destination):
    own_count = orbitals.shape[0]
    slot_count = own_count + own_count // 2
    me = lax.axis_index("pts").astype(jnp.int32)
    group_count = lax.axis_size("pts")
    half = group_count // 2
    me_ref = me.reshape(1)
    low = (me % half).reshape(1)

    order = []
    bit = half
    near = orbitals
    while bit > 1:
        near = jnp.concatenate([near, swap(near, bit)], axis=0)
        order.append(bit)
        bit //= 2
    far = swap(near, 1)
    rows = place_orbitals(near, far, destination, me_ref, slot_count, group_count, own_count, order)

    early, late = gather_points(points, half)

    values = field_values(fields)
    weights_here = jnp.einsum("wg,pg->wp", values, coupling, preferred_element_type=jnp.float32)
    sends = slot_scales(weights_here, destination, me_ref, slot_count, group_count)
    halves = [list(range(half)), list(range(half, group_count))]
    scales = lax.all_to_all(sends, "pts", split_axis=0, concat_axis=0, tiled=True, axis_index_groups=halves)

    part = image(rows, low, scales, early, "first_early") + image(rows, low, scales, late, "first_late")
    part = rotate(part)
    sent = part.astype(jnp.bfloat16)
    for_theirs = swap(sent[:slot_count], half)
    for_own = swap(sent[slot_count:], half)
    first_own = part[:slot_count] + for_own.astype(jnp.float32)
    first_theirs = part[slot_count:] + for_theirs.astype(jnp.float32)
    pieces = early + late
    scales_own, scales_theirs = scales[:, :slot_count], scales[:, slot_count:]
    image_theirs = image(first_theirs.astype(jnp.bfloat16), low, scales_theirs, pieces, "second_theirs")
    arrived = swap(image_theirs.astype(jnp.bfloat16), half)
    image_own = image(first_own.astype(jnp.bfloat16), low, scales_own, pieces, "second_own")
    second = 0.5 * rotate(image_own + arrived.astype(jnp.float32))
    return (rows[:slot_count].astype(jnp.float32) + first_own + second).astype(jnp.bfloat16)


def solution(mesh):
    return jax.shard_map(
        per_device,
        mesh=mesh,
        in_specs=(
            P(("rep", "pts"), None, None),
            P("pts", None),
            P("pts", None),
            P("rep", None),
            P("rep"),
        ),
        out_specs=P(("rep", "pts"), None, None),
        check_vma=False,
    )
```

```python
import functools

import jax
import jax.numpy as jnp
from jax import lax
from jax.experimental import pallas as pl
from jax.experimental.pallas import tpu as pltpu
from jax.sharding import PartitionSpec as P


LEVELS = (-2.3344142183389773, -0.7419637843027258, 0.7419637843027258, 2.3344142183389773)
VMEM = pl.BlockSpec(memory_space=pltpu.VMEM)
SMEM = pl.BlockSpec(memory_space=pltpu.SMEM)
PARAMS = pltpu.CompilerParams(vmem_limit_bytes=24 * 1024 * 1024)


def field_values(fields):
    values = jnp.zeros(fields.shape, jnp.float32)
    for level_index in range(4):
        values = values + jnp.where(fields == level_index, LEVELS[level_index], 0.0)
    return values.astype(jnp.bfloat16)


def swap(block, offset):
    count = lax.axis_size("pts")
    return lax.ppermute(block, "pts", [(i, i ^ offset) for i in range(count)])


def fill_sources(dest_ref, source_ref, seen_ref, slot_count):
    def clear_slot(i, _):
        source_ref[i] = -1
        return 0

    def clear_seen(i, _):
        seen_ref[i] = 0
        return 0

    def place(walker, _):
        group = dest_ref[walker]
        rank = seen_ref[group]
        seen_ref[group] = rank + 1
        source_ref[group * slot_count + rank] = walker
        return 0

    lax.fori_loop(0, source_ref.shape[0], clear_slot, 0)
    lax.fori_loop(0, seen_ref.shape[0], clear_seen, 0)
    lax.fori_loop(0, dest_ref.shape[0], place, 0)


def scale_slots_kernel(slot_count, group_count, dest_ref, me_ref, scale_ref, out_ref, source_ref, seen_ref):
    fill_sources(dest_ref, source_ref, seen_ref, slot_count)
    half = group_count // 2
    top = me_ref[0] // half
    for group in range(half):
        for member in range(2):
            owner = (top ^ member) * half + group
            for k in range(slot_count):
                walker = jnp.maximum(source_ref[owner * slot_count + k], 0)
                row = scale_ref[pl.ds(walker, 1), :]
                out_ref[group, pl.ds(member * slot_count + k, 1), :] = row


def slot_scales(scale, destination, me, slot_count, group_count):
    slots = 2 * slot_count
    return pl.pallas_call(
        functools.partial(scale_slots_kernel, slot_count, group_count),
        out_shape=jax.ShapeDtypeStruct((group_count // 2, slots, scale.shape[1]), jnp.float32),
        in_specs=[SMEM, SMEM, VMEM],
        out_specs=VMEM,
        scratch_shapes=[
            pltpu.SMEM((group_count * slot_count,), jnp.int32),
            pltpu.SMEM((group_count,), jnp.int32),
        ],
        compiler_params=PARAMS,
        name="slot_scales",
    )(destination, me, scale)


def place_kernel(slot_count, group_count, own_count, order, dest_ref, me_ref, near_ref, far_ref, out_ref, source_ref, seen_ref):
    fill_sources(dest_ref, source_ref, seen_ref, slot_count)
    half = group_count // 2
    me = me_ref[0]
    for member in range(2):
        for k in range(slot_count):
            owner = me ^ (half * member)
            walker = source_ref[owner * slot_count + k]
            slot = member * slot_count + k

            @pl.when(walker < 0)
            def _():
                out_ref[slot] = jnp.zeros(out_ref.shape[1:], out_ref.dtype)

            @pl.when(walker >= 0)
            def _():
                offset = (walker // own_count) ^ me
                place = jnp.int32(0)
                for step, bit in enumerate(order):
                    place = place + ((offset // bit) & 1) * (1 << step)
                place = place * own_count + walker % own_count

                @pl.when((offset & 1) == 0)
                def _():
                    out_ref[slot] = near_ref[place]

                @pl.when((offset & 1) == 1)
                def _():
                    out_ref[slot] = far_ref[place]


def place_orbitals(near, far, destination, me, slot_count, group_count, own_count, order):
    slots = 2 * slot_count
    return pl.pallas_call(
        functools.partial(place_kernel, slot_count, group_count, own_count, order),
        out_shape=jax.ShapeDtypeStruct((slots,) + near.shape[1:], near.dtype),
        in_specs=[SMEM, SMEM, VMEM, VMEM],
        out_specs=VMEM,
        scratch_shapes=[
            pltpu.SMEM((group_count * slot_count,), jnp.int32),
            pltpu.SMEM((group_count,), jnp.int32),
        ],
        compiler_params=PARAMS,
        name="place_orbitals",
    )(destination, me, near, far)


def image_of(rows, low, scale_ref, pieces):
    slots, per_slot, orbs = rows.shape
    flat = rows.reshape(slots * per_slot, orbs)
    total = jnp.zeros((slots * per_slot, orbs), jnp.float32)
    for offset, begin, ref in pieces:
        table = ref[...]
        count = table.shape[0]
        inner = lax.dot_general(flat, table, (((1,), (1,)), ((), ())), preferred_element_type=jnp.float32)
        scale = scale_ref[low ^ offset][:, begin:begin + count]
        scaled = inner.reshape(slots, per_slot, count) * scale[:, None, :]
        scaled = scaled.astype(jnp.bfloat16).reshape(slots * per_slot, count)
        total = total + jnp.dot(scaled, table, preferred_element_type=jnp.float32)
    return total.reshape(slots, per_slot, orbs)


def image_kernel(keys, low_ref, rows_ref, scale_ref, *refs):
    out_ref = refs[-1]
    low = low_ref[0]
    pieces = [(offset, begin, ref) for (offset, begin), ref in zip(keys, refs)]
    out_ref[...] = image_of(rows_ref[...], low, scale_ref, pieces)


def image(rows, low, scales, pieces):
    keys = [(m, begin) for m, begin, _, _ in pieces]
    points_count = sum(p.shape[0] for *_, p in pieces)
    flops = 4 * rows.shape[0] * rows.shape[1] * rows.shape[2] * points_count
    return pl.pallas_call(
        functools.partial(image_kernel, keys),
        out_shape=jax.ShapeDtypeStruct(rows.shape, jnp.float32),
        in_specs=[SMEM] + [VMEM] * (2 + len(pieces)),
        out_specs=VMEM,
        compiler_params=PARAMS,
        cost_estimate=pl.CostEstimate(flops=flops, bytes_accessed=points_count * rows.shape[2] * 2, transcendentals=0),
    )(low, rows, scales, *[p for *_, p in pieces])


def rotate(block):
    half_rows = block.shape[-2] // 2
    return jnp.concatenate([-block[..., half_rows:, :], block[..., :half_rows, :]], axis=-2)


def gather_points(points, half):
    early, late = [(0, 0, "p0", points)], []
    bits = []
    bit = 2
    while bit < half:
        bits.append(bit)
        bit *= 2
    if len(bits) >= 2:
        one, two = bits[:2]
        middle = points.shape[0] // 2
        low, high = points[:middle], points[middle:]
        one_low = swap(low, one)
        two_high = swap(high, two)
        one_high = swap(high, one)
        two_low = swap(low, two)
        early += [
            (one, 0, "one_low", one_low),
            (two, middle, "two_high", two_high),
            (one, middle, "one_high", one_high),
            (two, 0, "two_low", two_low),
        ]
        late += [(one ^ two, 0, "both_low", swap(one_low, two)), (one ^ two, middle, "both_high", swap(two_high, one))]
        bits = bits[2:]
    for bit in bits:
        late += [(m ^ bit, begin, f"{name}_{bit}", swap(rows, bit)) for m, begin, name, rows in early + late]

    def far(pieces):
        return [(m ^ 1, begin, f"{name}_far", swap(rows, 1)) for m, begin, name, rows in pieces]

    return early + far(early), late + far(late)


def step(orbitals, points, coupling, fields, destination):
    own_count = orbitals.shape[0]
    slot_count = own_count + own_count // 2
    me = lax.axis_index("pts").astype(jnp.int32)
    group_count = lax.axis_size("pts")
    half = group_count // 2
    me_ref = me.reshape(1)
    low = (me % half).reshape(1)

    order = []
    bit = half
    near = orbitals
    while bit > 1:
        near = jnp.concatenate([near, swap(near, bit)], axis=0)
        order.append(bit)
        bit //= 2
    far = swap(near, 1)
    rows = place_orbitals(near, far, destination, me_ref, slot_count, group_count, own_count, order)

    early, late = gather_points(points, half)

    values = field_values(fields)
    weights_here = jnp.einsum("wg,pg->wp", values, coupling, preferred_element_type=jnp.float32)
    sends = slot_scales(weights_here, destination, me_ref, slot_count, group_count)
    halves = [list(range(half)), list(range(half, group_count))]
    scales = lax.all_to_all(sends, "pts", split_axis=0, concat_axis=0, tiled=True, axis_index_groups=halves)

    part = image(rows, low, scales, early)
    part = part + image(rows, low, scales, late)
    part = rotate(part)
    sent = part.astype(jnp.bfloat16)
    for_theirs = swap(sent[:slot_count], half)
    for_own = swap(sent[slot_count:], half)
    pieces = early + late
    scales_own, scales_theirs = scales[:, :slot_count], scales[:, slot_count:]
    first_theirs = part[slot_count:] + for_theirs.astype(jnp.float32)
    image_theirs = image(first_theirs.astype(jnp.bfloat16), low, scales_theirs, pieces)
    image_theirs, for_own = lax.optimization_barrier((image_theirs, for_own))
    arrived = swap(image_theirs.astype(jnp.bfloat16), half)
    first_own = part[:slot_count] + for_own.astype(jnp.float32)
    image_own = image(first_own.astype(jnp.bfloat16), low, scales_own, pieces)
    second = 0.5 * rotate(image_own + arrived.astype(jnp.float32))
    return (rows[:slot_count].astype(jnp.float32) + first_own + second).astype(jnp.bfloat16)


def solution(mesh):
    return jax.shard_map(
        step,
        mesh=mesh,
        in_specs=(
            P(("rep", "pts"), None, None),
            P("pts", None),
            P("pts", None),
            P("rep", None),
            P("rep"),
        ),
        out_specs=P(("rep", "pts"), None, None),
        check_vma=False,
    )
```
